32 devices in a mesh: grp: 2 (over y), seq: 4 (over z), ch: 2 (over x), col: 2 (over core).
Axes of the slice: x: 2, y: 2, z: 4, core: 2. Of those that a mesh axis runs over, the one named last changes fastest.
Arguments:
- latent: bfloat16 [8, 4, 16, 512], P('grp', 'seq', 'col', 'ch'), parts along dimension 0, may hold values from -8 to 8, as said below
- mid_gain: float32 [512], P('ch'), may hold values from 0.25 to 1.75
- mid_bias: float32 [512], P('ch'), may hold values from -3 to 3
- mid_weight: bfloat16 [3, 3, 3, 512, 512], P(None, None, None, None, 'ch'), may hold values from -0.0546875 to 0.0546875
- mid_conv_bias: float32 [512], P('ch'), may hold values from -2 to 2
- first_gain: float32 [512], P('ch'), may hold values from 0.25 to 1.75
- first_bias: float32 [512], P('ch'), may hold values from -3 to 3
- first_weight: bfloat16 [3, 3, 3, 512, 512], P(None, None, None, None, 'ch'), may hold values from -0.0546875 to 0.0546875
- first_conv_bias: float32 [512], P('ch'), may hold values from -2 to 2
- second_gain: float32 [512], P('ch'), may hold values from 0.25 to 1.75
- second_bias: float32 [512], P('ch'), may hold values from -3 to 3
- second_weight: bfloat16 [3, 3, 3, 512, 512], P(None, None, None, None, 'ch'), may hold values from -0.0546875 to 0.0546875
- second_conv_bias: float32 [512], P('ch'), may hold values from -2 to 2
Outputs:
- decoded: bfloat16 [16, 4, 16, 512], P(('grp', 'seq'), None, 'col', 'ch'), parts along dimension 0
The draws below stay inside these ranges and needn't reach their ends.
There are 2 independent parts, one for each index of `grp`. The reference program is written for one: setup_inputs(seed, part) draws one part's arguments, and reference() takes and returns one part's arrays. A program takes and returns all parts, laid end to end along the dimension named above; an argument that names none is the same for every part. Nothing has to cross between parts.
Inputs may be any that keep to these rules, and one draw needn't show every extreme that they name: `latent`: each row has its own scale and each row and channel its own offset; values are clipped to the range.
All inputs are finite; a program needn't handle non-finite values.
Results may differ from the reference program's by a relative error of at most 0.0095.
Values may be sent and summed in bfloat16 or wider, within the bound.
A program may use at most 64 MiB of HBM per device.

```python
import jax
import jax.numpy as jnp
from jax import lax

C = 512
GROUPS = 32
FRAMES = 4
HEIGHT = 4
WIDTH = 16


def draw_latent(key, part):
    first_key, second_key, third_key = jax.random.split(jax.random.fold_in(key, 17), 3)
    gauss_noise = jax.random.normal(first_key, (FRAMES, HEIGHT, WIDTH, C), jnp.float32)
    row_scale = jnp.exp(jax.random.uniform(second_key, (1, HEIGHT, 1, 1), jnp.float32, -0.7, 0.7))
    offset = 0.5 * jax.random.normal(third_key, (1, HEIGHT, 1, C), jnp.float32)
    return jnp.clip(gauss_noise * row_scale + offset, -8.0, 8.0).astype(jnp.bfloat16)


def block_scale(key, extent, shards, least, largest):
    level, own = 1.0, jax.random.fold_in(key, 6)
    for dim, blocks in shards:
        steps = jnp.exp(jax.random.uniform(jax.random.fold_in(own, dim), (blocks,), jnp.float32, least / len(shards), largest / len(shards)))
        level = level * jnp.repeat(steps, extent[dim] // blocks).reshape([-1 if axis == dim else 1 for axis in range(len(extent))])
    return level


def noise(rng, dims, scale, limit, cuts=(), kind=jnp.bfloat16):
    level = block_scale(rng, dims, cuts, -0.22, 0.18) if cuts else 1.0
    drawn = jax.random.normal(rng, dims, jnp.float32) * scale * level
    return jnp.minimum(jnp.maximum(drawn, -limit), limit).astype(kind)


def setup_inputs(seed: int = 0, part: int = 0) -> dict:
    seeds = jax.random.split(jax.random.key(seed), 14)
    own_keys = jax.random.split(jax.random.fold_in(seeds[13], part), 14)
    return {
        "latent": draw_latent(jax.random.fold_in(jax.random.fold_in(seeds[13], part), 71), part),
        "mid_gain": jnp.clip(1.0 + 0.15 * jax.random.normal(seeds[1], (C,), jnp.float32), 0.25, 1.75),
        "mid_bias": noise(seeds[2], (C,), 0.5, 3.0, ((0, 2),), jnp.float32),
        "mid_weight": noise(seeds[3], (3, 3, 3, C, C), (27 * C) ** -0.5, 0.0546875, ((4, 2),)),
        "mid_conv_bias": noise(seeds[4], (C,), 0.3, 2.0, ((0, 2),), jnp.float32),
        "first_gain": jnp.clip(1.0 + 0.15 * jax.random.normal(seeds[5], (C,), jnp.float32), 0.25, 1.75),
        "first_bias": noise(seeds[6], (C,), 0.5, 3.0, ((0, 2),), jnp.float32),
        "first_weight": noise(seeds[7], (3, 3, 3, C, C), (27 * C) ** -0.5, 0.0546875, ((4, 2),)),
        "first_conv_bias": noise(seeds[8], (C,), 0.3, 2.0, ((0, 2),), jnp.float32),
        "second_gain": jnp.clip(1.0 + 0.15 * jax.random.normal(seeds[9], (C,), jnp.float32), 0.25, 1.75),
        "second_bias": noise(seeds[10], (C,), 0.5, 3.0, ((0, 2),), jnp.float32),
        "second_weight": noise(seeds[11], (3, 3, 3, C, C), (27 * C) ** -0.5, 0.0546875, ((4, 2),)),
        "second_conv_bias": noise(seeds[12], (C,), 0.3, 2.0, ((0, 2),), jnp.float32),
    }


def group_norm(field, gain, shift_term):
    values = field.astype(jnp.float32)
    group_size = C // GROUPS
    totals = lax.optimization_barrier(jnp.sum(values, axis=(0, 1, 2))).reshape(GROUPS, group_size).sum(axis=1)
    squares = lax.optimization_barrier(jnp.sum(values * values, axis=(0, 1, 2))).reshape(GROUPS, group_size).sum(axis=1)
    samples = values.shape[0] * values.shape[1] * values.shape[2] * group_size
    group_mean = totals / samples
    spread = squares / samples - group_mean * group_mean
    inverse = 1.0 / jnp.sqrt(spread + 0.01)
    scaled = (values - jnp.repeat(group_mean, group_size)) * jnp.repeat(inverse, group_size) * gain + shift_term
    return jax.nn.silu(scaled).astype(jnp.bfloat16)

def convolve(field, weight):
    result = lax.conv_general_dilated(field[None].astype(jnp.float32), weight.astype(jnp.float32), (1, 1, 1), ((2, 0), (1, 1), (1, 1)), dimension_numbers=('NDHWC', 'DHWIO', 'NDHWC'), precision=lax.Precision.HIGHEST)
    return result[0]

def reference(latent, mid_gain, mid_bias, mid_weight, mid_conv_bias, first_gain, first_bias, first_weight, first_conv_bias, second_gain, second_bias, second_weight, second_conv_bias):
    mid_act = group_norm(latent, mid_gain, mid_bias)
    middle = (latent.astype(jnp.float32) + convolve(mid_act, mid_weight) + mid_conv_bias).astype(jnp.bfloat16)
    doubled = jnp.repeat(middle, 2, axis=0)
    first_act = group_norm(doubled, first_gain, first_bias)
    hidden = (convolve(first_act, first_weight) + first_conv_bias).astype(jnp.bfloat16)
    second_act = group_norm(hidden, second_gain, second_bias)
    return (doubled.astype(jnp.float32) + convolve(second_act, second_weight) + second_conv_bias).astype(jnp.bfloat16)
```

```python
import functools

import jax
import jax.numpy as jnp
from jax import lax
from jax.experimental import pallas as pl
from jax.experimental.pallas import tpu as pltpu
from jax.sharding import PartitionSpec as P

GROUPS = 32
MESH = pl.DeviceIdType.MESH
F32 = jnp.float32
BF16 = jnp.bfloat16


def each(count, visit):
    if count <= 16:
        for i in range(count):
            visit(i)
    else:
        lax.fori_loop(0, count, lambda i, carry: (visit(i), carry)[1], 0)


def kernel(
    sizes,
    latent,
    mid_gain, mid_bias, mid_conv_bias,
    first_gain, first_bias, first_conv_bias,
    second_gain, second_bias, second_conv_bias,
    mid_weight, first_weight, second_weight,
    out,
    w0, w1, w2, w_sem,
    act0, act1, act2,
    params, stat, packed, group_ref,
    lat, lat_edge_src, lat_edge,
    mid_src, mid_edge_src, mid, mid_edge,
    hid_src, hid_edge_src, hid, hid_edge,
    par_send, par_recv, stat_send, stat_recv,
    lat_send, lat_recv, late_send, late_recv,
    mid_send, mid_recv, mide_send, mide_recv,
    hid_send, hid_recv, hide_send, hide_recv,
):
    ns, nh, nk, frames, width, chans, group_size = sizes
    rows = ns
    n, pairs, spread_over = ns * nh * nk, ns * nh, ns * nk
    s, h, k = lax.axis_index("seq"), lax.axis_index("ch"), lax.axis_index("col")
    other = 1 - k
    me = h * spread_over + s * nk + k

    def coords(flat):
        return {"ch": flat // spread_over, "seq": (flat % spread_over) // nk, "col": flat % nk}

    barrier = pltpu.get_barrier_semaphore()

    def greet(i):
        pl.semaphore_signal(barrier, inc=1, device_id=coords((me + i + 1) % n), device_id_type=MESH)

    each(n - 1, greet)

    loads = []
    for c, (source, target) in enumerate(((mid_weight, w0), (first_weight, w1), (second_weight, w2))):
        for dt in range(3):
            load = pltpu.make_async_copy(source.at[dt], target.at[dt], w_sem.at[c, dt])
            load.start()
            loads.append(load)

    def send(src, dst, send_sem, recv_sem, where):
        pltpu.make_async_remote_copy(
            src_ref=src, dst_ref=dst, send_sem=send_sem, recv_sem=recv_sem,
            device_id=where, device_id_type=MESH,
        ).start()

    def take(ref, sem):
        pltpu.make_async_copy(ref, ref, sem).wait()

    def own_stats(step, values):
        flat = values.reshape(-1, chans)
        stat[step, me, 0:1, :] = jnp.sum(flat, axis=0, keepdims=True)
        stat[step, me, 1:2, :] = jnp.sum(flat * flat, axis=0, keepdims=True)

    def send_stats(step):
        def visit(i):
            send(stat.at[step, me], stat.at[step, me], stat_send.at[step], stat_recv.at[step],
                 coords((me + i + 1) % n))
        each(n - 1, visit)

    def edge_of(values):
        return jnp.where(k == 0, values[:, width - 1:width, :], values[:, 0:1, :])

    tile = latent[...].reshape(frames, width, chans)
    values = tile.astype(F32)
    lat[1, h] = tile
    lat_edge_src[...] = edge_of(values)
    own_stats(0, values)
    for row, ref in enumerate((mid_gain, mid_bias, first_gain, first_bias, second_gain, second_bias)):
        params[h, row:row + 1, :] = ref[...].reshape(1, chans)

    pl.semaphore_wait(barrier, n - 1)

    send_stats(0)
    for d in range(1, nh):
        there = {"seq": s, "ch": (h + d) % nh, "col": k}
        send(params.at[h], params.at[h], par_send, par_recv, there)

    def near(steps, ring):
        if steps == 0:
            ring()
        else:
            pl.when((s + steps >= 0) & (s + steps < ns))(ring)

    for slot in range(3):
        def ring(slot=slot):
            steps = 1 - slot
            for d in range(0 if steps else 1, nh):
                there = {"seq": s + steps, "ch": (h + d) % nh, "col": k}
                send(lat.at[1, h], lat.at[slot, h], lat_send.at[slot], lat_recv.at[slot], there)
            for d in range(nh):
                there = {"seq": s + steps, "ch": (h + d) % nh, "col": other}
                send(lat_edge_src, lat_edge.at[slot, h], late_send.at[slot], late_recv.at[slot], there)
        near(1 - slot, ring)

    act0[...] = jnp.zeros_like(act0)
    act1[...] = jnp.zeros_like(act1)
    act2[...] = jnp.zeros_like(act2)
    packed[...] = jnp.zeros_like(packed)
    mid_src[0] = jnp.zeros((width, chans), BF16)
    mid_edge_src[0] = jnp.zeros((1, chans), F32)
    here = lax.broadcasted_iota(jnp.int32, (chans, chans), 0) // group_size
    there = lax.broadcasted_iota(jnp.int32, (chans, chans), 1) // group_size
    group_ref[...] = jnp.where(here == there, 1.0, 0.0).astype(BF16)

    def norm_terms(step, samples):
        take(stat.at[step, pl.ds(0, n - 1)], stat_recv.at[step])
        for j in range(nh):
            packed[2 * j:2 * j + 2, :] = jnp.sum(stat[step, j * spread_over:(j + 1) * spread_over], axis=0)
        exact = packed[...]
        high = exact.astype(BF16)
        rest = exact - high.astype(F32)
        middle = rest.astype(BF16)
        low = (rest - middle.astype(F32)).astype(BF16)
        group = group_ref[...]
        total = sum(jnp.dot(part, group, preferred_element_type=F32) for part in (low, middle, high))
        terms = []
        for j in range(nh):
            mean = total[2 * j:2 * j + 1] / samples
            square = total[2 * j + 1:2 * j + 2] / samples
            inverse = 1.0 / jnp.sqrt(square - mean * mean + 0.01)
            gain = params[j, 2 * step:2 * step + 1, :]
            shift = params[j, 2 * step + 1:2 * step + 2, :]
            terms.append((mean, inverse * gain, shift))
        return terms

    def activate(values, term):
        mean, scale, shift = term
        scaled = (values.astype(F32) - mean) * scale + shift
        return scaled / (1.0 + jnp.exp(-scaled))

    def place(target, index, j, values, edge, term):
        centre = activate(values, term)
        side = activate(edge, term)
        left = jnp.where(k == 1, side, 0.0)
        right = jnp.where(k == 0, side, 0.0)
        column = lax.broadcasted_iota(jnp.int32, centre.shape, 1)
        lanes = slice(j * chans, (j + 1) * chans)
        before = jnp.where(column == 0, left, pltpu.roll(centre, 1, 1))
        after = jnp.where(column == width - 1, right, pltpu.roll(centre, width - 1, 1))
        for dj, moved in enumerate((before, centre, after)):
            target[(dj,) + index + (slice(None), lanes)] = moved

    def taps(window, weight, dt):
        total = None
        for di in range(3):
            for dj in range(3):
                lhs = window(di, dj)
                lhs = lhs.reshape(-1, lhs.shape[-1]).astype(BF16)
                part = jnp.dot(lhs, weight[dt, di, dj], preferred_element_type=F32)
                total = part if total is None else total + part
        return total

    take(params.at[pl.ds(0, nh - 1)], par_recv)
    terms = norm_terms(0, frames * width * group_size * spread_over)
    for slot in range(3):
        def fill(slot=slot):
            if slot == 1:
                take(lat.at[slot, pl.ds(0, nh - 1)], lat_recv.at[slot])
            else:
                take(lat.at[slot], lat_recv.at[slot])
            take(lat_edge.at[slot], late_recv.at[slot])
            for j in range(nh):
                place(act0, (slice(2, 2 + frames), slot), j, lat[slot, j], lat_edge[slot, j], terms[j])
        near(slot - 1, fill)
    mixed = None
    for dt in range(3):
        loads[dt].wait()
        part = taps(lambda di, dj: act0[dj, dt:dt + frames, di], w0, dt)
        mixed = part if mixed is None else mixed + part
    summed = values.reshape(-1, chans) + mixed + mid_conv_bias[...].reshape(1, chans)
    tile = summed.astype(BF16).reshape(frames, width, chans)
    values = tile.astype(F32)
    mid_src[1:1 + frames] = tile
    mid_edge_src[1:1 + frames] = edge_of(values)
    own_stats(1, values)
    slot_here = h * ns + s

    def send_mid(i):
        q = (slot_here + i + 1) % pairs
        send(mid_src.at[pl.ds(q % ns, 2)], mid.at[slot_here], mid_send, mid_recv,
             {"seq": q % ns, "ch": q // ns, "col": k})

    def send_mid_edge(i):
        q = (slot_here + i) % pairs
        send(mid_edge_src.at[pl.ds(q % ns, 2)], mid_edge.at[slot_here], mide_send, mide_recv,
             {"seq": q % ns, "ch": q // ns, "col": other})

    each(pairs - 1, send_mid)
    each(pairs, send_mid_edge)
    send_stats(1)
    mid[slot_here] = mid_src[pl.ds(s, 2)]

    terms = norm_terms(1, frames * width * group_size * spread_over)
    take(mid.at[pl.ds(0, pairs - 1)], mid_recv)
    take(mid_edge, mide_recv)

    def fill_frame(f):
        for j in range(nh):
            place(act1, (f, slice(1, 1 + rows)), j, mid[j * ns:(j + 1) * ns, f],
                  mid_edge[j * ns:(j + 1) * ns, f], terms[j])

    pl.when(s > 0)(lambda: fill_frame(0))
    fill_frame(1)
    for dt in range(3):
        loads[3 + dt].wait()
    half = rows * width
    oldest = taps(lambda di, dj: act1[dj, 0, di:di + rows], w1, 0)
    both = taps(lambda di, dj: act1[dj, :, di:di + rows], w1, 1)
    newest = taps(lambda di, dj: act1[dj, 1, di:di + rows], w1, 2)
    shared = oldest + newest + first_conv_bias[...].reshape(1, chans)
    summed = jnp.concatenate([shared + both[:half], shared + both[half:]], axis=0)
    tile = summed.astype(BF16).reshape(2 * rows, width, chans)
    values = tile.astype(F32)
    hid_src[...] = tile
    hid_edge_src[...] = edge_of(values)
    own_stats(2, values)
    for slot in (1, 0):
        def ring(slot=slot):
            steps = 1 - slot
            for d in range(0 if steps else 1, nh):
                there = {"seq": s + steps, "ch": (h + d) % nh, "col": k}
                send(hid_src, hid.at[slot, h], hid_send.at[slot], hid_recv.at[slot], there)
            for d in range(nh):
                there = {"seq": s + steps, "ch": (h + d) % nh, "col": other}
                send(hid_edge_src, hid_edge.at[slot, h], hide_send.at[slot], hide_recv.at[slot], there)
        near(1 - slot, ring)
    send_stats(2)
    hid[1, h] = tile

    terms = norm_terms(2, 2 * rows * width * group_size * spread_over)
    for slot in (1, 0):
        def fill(slot=slot):
            if slot == 1:
                take(hid.at[slot, pl.ds(0, nh - 1)], hid_recv.at[slot])
            else:
                take(hid.at[slot], hid_recv.at[slot])
            take(hid_edge.at[slot], hide_recv.at[slot])
            for j in range(nh):
                for f in range(2):
                    part = slice(f * rows, (f + 1) * rows)
                    place(act2, (2 * slot + f, slice(1, 1 + rows)), j, hid[slot, j, part],
                          hid_edge[slot, j, part], terms[j])
        near(slot - 1, fill)
    mixed = None
    for dt in range(3):
        loads[6 + dt].wait()
        part = taps(lambda di, dj: act2[dj, dt:dt + 2, di:di + rows], w2, dt)
        mixed = part if mixed is None else mixed + part
    mixed = mixed + second_conv_bias[...].reshape(1, chans)
    kept = mid[pl.ds(h * ns, ns), 1].astype(F32).reshape(half, chans)
    for f in range(2):
        whole = kept + mixed[f * half:(f + 1) * half]
        out[f] = whole.astype(BF16).reshape(rows, width, chans)

    for step in range(3):
        take(stat.at[step, pl.ds(0, n - 1)], stat_send.at[step])
    take(params.at[pl.ds(0, nh - 1)], par_send)
    take(mid.at[pl.ds(0, pairs - 1)], mid_send)
    take(mid_edge, mide_send)
    for slot in range(3):
        def left(slot=slot):
            if slot == 1:
                take(lat.at[slot, pl.ds(0, nh - 1)], lat_send.at[slot])
            else:
                take(lat.at[slot], lat_send.at[slot])
            take(lat_edge.at[slot], late_send.at[slot])
        near(1 - slot, left)
    for slot in (1, 0):
        def left(slot=slot):
            if slot == 1:
                take(hid.at[slot, pl.ds(0, nh - 1)], hid_send.at[slot])
            else:
                take(hid.at[slot], hid_send.at[slot])
            take(hid_edge.at[slot], hide_send.at[slot])
        near(1 - slot, left)


def solution(mesh):
    ns, nh, nk = mesh.shape["seq"], mesh.shape["ch"], mesh.shape["col"]

    def body(
        latent,
        mid_gain, mid_bias, mid_weight, mid_conv_bias,
        first_gain, first_bias, first_weight, first_conv_bias,
        second_gain, second_bias, second_weight, second_conv_bias,
    ):
        frames, own_rows, width, chans = latent.shape
        assert nk == 2 and own_rows == 1 and frames == ns
        rows = ns
        full = chans * nh
        sizes = (ns, nh, nk, frames, width, chans, full // GROUPS)
        n, pairs = ns * nh * nk, ns * nh
        vmem = pl.BlockSpec(memory_space=pltpu.VMEM)
        hbm = pl.BlockSpec(memory_space=pl.ANY)
        dma = pltpu.SemaphoreType.DMA
        taps = mid_weight.shape
        return pl.pallas_call(
            functools.partial(kernel, sizes),
            out_shape=jax.ShapeDtypeStruct((2, rows, width, chans), BF16),
            in_specs=[vmem] * 10 + [hbm] * 3,
            out_specs=vmem,
            scratch_shapes=[
                pltpu.VMEM(taps, BF16), pltpu.VMEM(taps, BF16), pltpu.VMEM(taps, BF16), dma((3, 3)),
                pltpu.VMEM((3, frames + 2, 3, width, full), F32),
                pltpu.VMEM((3, 2, rows + 2, width, full), F32),
                pltpu.VMEM((3, 4, rows + 2, width, full), F32),
                pltpu.VMEM((nh, 8, chans), F32),
                pltpu.VMEM((3, n, 2, chans), F32),
                pltpu.VMEM((max(8, 2 * nh), chans), F32),
                pltpu.VMEM((chans, chans), BF16),
                pltpu.VMEM((3, nh, frames, width, chans), BF16),
                pltpu.VMEM((frames, 1, chans), F32),
                pltpu.VMEM((3, nh, frames, 1, chans), F32),
                pltpu.VMEM((frames + 1, width, chans), BF16),
                pltpu.VMEM((frames + 1, 1, chans), F32),
                pltpu.VMEM((pairs, 2, width, chans), BF16),
                pltpu.VMEM((pairs, 2, 1, chans), F32),
                pltpu.VMEM((2 * rows, width, chans), BF16),
                pltpu.VMEM((2 * rows, 1, chans), F32),
                pltpu.VMEM((2, nh, 2 * rows, width, chans), BF16),
                pltpu.VMEM((2, nh, 2 * rows, 1, chans), F32),
                dma, dma, dma((3,)), dma((3,)),
                dma((3,)), dma((3,)), dma((3,)), dma((3,)),
                dma, dma, dma, dma,
                dma((2,)), dma((2,)), dma((2,)), dma((2,)),
            ],
            compiler_params=pltpu.CompilerParams(
                collective_id=0, has_side_effects=True, vmem_limit_bytes=60 * 1024 * 1024
            ),
        )(
            latent,
            mid_gain, mid_bias, mid_conv_bias,
            first_gain, first_bias, first_conv_bias,
            second_gain, second_bias, second_conv_bias,
            mid_weight, first_weight, second_weight,
        )

    vector, weight = P("ch"), P(None, None, None, None, "ch")
    in_specs = (P("grp", "seq", "col", "ch"),) + (vector, vector, weight, vector) * 3
    out_specs = P(("grp", "seq"), None, "col", "ch")
    return jax.shard_map(body, mesh=mesh, in_specs=in_specs, out_specs=out_specs, check_vma=False)
```

```python
import functools

import jax
import jax.numpy as jnp
from jax import lax
from jax.experimental import pallas as pl
from jax.experimental.pallas import tpu as pltpu
from jax.sharding import PartitionSpec as P

GROUPS = 32
MESH = pl.DeviceIdType.MESH
F32 = jnp.float32
BF16 = jnp.bfloat16


def each(count, visit):
    if count <= 4:
        for i in range(count):
            visit(i)
    else:
        lax.fori_loop(0, count, lambda i, carry: (visit(i), carry)[1], 0)


def kernel(
    sizes,
    *refs,
):
    smalls, (mid_weight, first_weight, second_weight), (out,) = refs[:10], refs[10:13], refs[13:14]
    latent, *vectors = refs[14:24]
    (mid_gain, mid_bias, mid_conv_bias, first_gain, first_bias, first_conv_bias,
     second_gain, second_bias, second_conv_bias) = vectors
    (
    small_sem,
    w0, w1, w2, w_sem,
    act0, act1, act2,
    params, stat, packed, group_ref,
    lat, lat_edge_src, lat_edge,
    mid_src, mid_edge_src, mid, mid_edge,
    hid_src, hid_edge_src, hid, hid_edge,
    par_send, par_recv, stat_send, stat_recv,
    lat_send, lat_recv, late_send, late_recv,
    mid_send, mid_recv, mide_send, mide_recv,
    hid_send, hid_recv, hide_send, hide_recv,
    ) = refs[24:]
    ns, nh, nk, frames, width, chans, group_size = sizes
    rows = ns
    n, pairs, spread_over = ns * nh * nk, ns * nh, ns * nk
    s, h, k = lax.axis_index("seq"), lax.axis_index("ch"), lax.axis_index("col")
    other = 1 - k
    me = h * spread_over + s * nk + k

    def wrap(index, count):
        return jnp.where(index >= count, index - count, index)

    def visit_all(visit):
        down = s < ns // 2
        def one(i):
            row = jnp.where(down, ns - 1 - i, i)
            for dh in reversed(range(nh)):
                for dk in range(nk):
                    visit(row, dh, dk)
        each(ns, one)

    def others(row, dh, dk, act):
        if dh == 0 and dk == 0:
            pl.when(row != s)(act)
        else:
            act()

    def place_of(row, dh, dk):
        return {"seq": row, "ch": wrap(h + dh, nh), "col": k if dk == 0 else other}

    barrier = pltpu.get_barrier_semaphore()

    def greet(row, dh, dk):
        others(row, dh, dk, lambda: pl.semaphore_signal(
            barrier, inc=1, device_id=place_of(row, dh, dk), device_id_type=MESH))

    visit_all(greet)
    small_loads = []
    for i, (source, target) in enumerate(zip(smalls, [latent] + vectors)):
        load = pltpu.make_async_copy(source, target, small_sem.at[i])
        load.start()
        small_loads.append(load)

    loads = []
    for c, (source, target) in enumerate(((mid_weight, w0), (first_weight, w1), (second_weight, w2))):
        for dt in range(3):
            load = pltpu.make_async_copy(source.at[dt], target.at[dt], w_sem.at[c, dt])
            load.start()
            loads.append(load)

    def send(src, dst, send_sem, recv_sem, where):
        pltpu.make_async_remote_copy(
            src_ref=src, dst_ref=dst, send_sem=send_sem, recv_sem=recv_sem,
            device_id=where, device_id_type=MESH,
        ).start()

    def take(ref, sem):
        pltpu.make_async_copy(ref, ref, sem).wait()

    def own_stats(step, values):
        flat = values.reshape(-1, chans)
        stat[step, me, 0:1, :] = jnp.sum(flat, axis=0, keepdims=True)
        stat[step, me, 1:2, :] = jnp.sum(flat * flat, axis=0, keepdims=True)

    def send_stats(step, row, dh, dk):
        others(row, dh, dk, lambda: send(
            stat.at[step, me], stat.at[step, me], stat_send.at[step], stat_recv.at[step],
            place_of(row, dh, dk)))

    def edge_of(values):
        return jnp.where(k == 0, values[:, width - 1:width, :], values[:, 0:1, :])

    for load in small_loads:
        load.wait()

    tile = latent[...].reshape(frames, width, chans)
    values = tile.astype(F32)
    lat[1, h] = tile
    lat_edge_src[...] = edge_of(values)
    own_stats(0, values)
    for row, ref in enumerate((mid_gain, mid_bias, first_gain, first_bias, second_gain, second_bias)):
        params[h, row:row + 1, :] = ref[...].reshape(1, chans)

    pl.semaphore_wait(barrier, n - 1)

    visit_all(functools.partial(send_stats, 0))
    for d in range(1, nh):
        there = {"seq": s, "ch": wrap(h + d, nh), "col": k}
        send(params.at[h], params.at[h], par_send, par_recv, there)

    def near(steps, ring):
        if steps == 0:
            ring()
        else:
            pl.when((s + steps >= 0) & (s + steps < ns))(ring)

    for slot in range(3):
        def ring(slot=slot):
            steps = 1 - slot
            for d in range(0 if steps else 1, nh):
                there = {"seq": s + steps, "ch": wrap(h + d, nh), "col": k}
                send(lat.at[1, h], lat.at[slot, h], lat_send.at[slot], lat_recv.at[slot], there)
            for d in range(nh):
                there = {"seq": s + steps, "ch": wrap(h + d, nh), "col": other}
                send(lat_edge_src, lat_edge.at[slot, h], late_send.at[slot], late_recv.at[slot], there)
        near(1 - slot, ring)

    act0[...] = jnp.zeros_like(act0)
    act1[...] = jnp.zeros_like(act1)
    act2[...] = jnp.zeros_like(act2)
    packed[...] = jnp.zeros_like(packed)
    mid_src[0] = jnp.zeros((width, chans), BF16)
    mid_edge_src[0] = jnp.zeros((1, chans), F32)
    here = lax.broadcasted_iota(jnp.int32, (chans, chans), 0) // group_size
    there = lax.broadcasted_iota(jnp.int32, (chans, chans), 1) // group_size
    group_ref[...] = jnp.where(here == there, 1.0, 0.0).astype(BF16)

    def norm_terms(step, samples):
        take(stat.at[step, pl.ds(0, n - 1)], stat_recv.at[step])
        for j in range(nh):
            packed[2 * j:2 * j + 2, :] = jnp.sum(stat[step, j * spread_over:(j + 1) * spread_over], axis=0)
        exact = packed[...]
        high = exact.astype(BF16)
        rest = exact - high.astype(F32)
        middle = rest.astype(BF16)
        low = (rest - middle.astype(F32)).astype(BF16)
        group = group_ref[...]
        total = sum(jnp.dot(part, group, preferred_element_type=F32) for part in (low, middle, high))
        terms = []
        for j in range(nh):
            mean = total[2 * j:2 * j + 1] / samples
            square = total[2 * j + 1:2 * j + 2] / samples
            inverse = 1.0 / jnp.sqrt(square - mean * mean + 0.01)
            gain = params[j, 2 * step:2 * step + 1, :]
            shift = params[j, 2 * step + 1:2 * step + 2, :]
            terms.append((mean, inverse * gain, shift))
        return terms

    def activate(values, term):
        mean, scale, shift = term
        scaled = (values.astype(F32) - mean) * scale + shift
        return scaled / (1.0 + jnp.exp(-scaled))

    def place(target, index, j, values, edge, term):
        centre = activate(values, term)
        side = activate(edge, term)
        left = jnp.where(k == 1, side, 0.0)
        right = jnp.where(k == 0, side, 0.0)
        column = lax.broadcasted_iota(jnp.int32, centre.shape, 1)
        lanes = slice(j * chans, (j + 1) * chans)
        before = jnp.where(column == 0, left, pltpu.roll(centre, 1, 1))
        after = jnp.where(column == width - 1, right, pltpu.roll(centre, width - 1, 1))
        for dj, moved in enumerate((before, centre, after)):
            target[(dj,) + index + (slice(None), lanes)] = moved

    def taps(window, weight, dt):
        total = None
        for di in range(3):
            for dj in range(3):
                lhs = window(di, dj)
                lhs = lhs.reshape(-1, lhs.shape[-1]).astype(BF16)
                part = jnp.dot(lhs, weight[dt, di, dj], preferred_element_type=F32)
                total = part if total is None else total + part
        return total

    take(params.at[pl.ds(0, nh - 1)], par_recv)
    terms = norm_terms(0, frames * width * group_size * spread_over)
    for slot in range(3):
        def fill(slot=slot):
            if slot == 1:
                take(lat.at[slot, pl.ds(0, nh - 1)], lat_recv.at[slot])
            else:
                take(lat.at[slot], lat_recv.at[slot])
            take(lat_edge.at[slot], late_recv.at[slot])
            for j in range(nh):
                place(act0, (slice(2, 2 + frames), slot), j, lat[slot, j], lat_edge[slot, j], terms[j])
        near(slot - 1, fill)
    mixed = None
    for dt in range(3):
        loads[dt].wait()
        part = taps(lambda di, dj: act0[dj, dt:dt + frames, di], w0, dt)
        mixed = part if mixed is None else mixed + part
    summed = values.reshape(-1, chans) + mixed + mid_conv_bias[...].reshape(1, chans)
    tile = summed.astype(BF16).reshape(frames, width, chans)
    values = tile.astype(F32)
    mid_src[1:1 + frames] = tile
    mid_edge_src[1:1 + frames] = edge_of(values)
    own_stats(1, values)
    slot_here = h * ns + s

    def send_mid(row, dh, dk):
        send_stats(1, row, dh, dk)
        if dk == 0:
            others(row, dh, dk, lambda: send(
                mid_src.at[pl.ds(row, 2)], mid.at[slot_here], mid_send, mid_recv, place_of(row, dh, dk)))
        else:
            send(mid_edge_src.at[pl.ds(row, 2)], mid_edge.at[slot_here], mide_send, mide_recv,
                 place_of(row, dh, dk))

    visit_all(send_mid)
    mid[slot_here] = mid_src[pl.ds(s, 2)]

    terms = norm_terms(1, frames * width * group_size * spread_over)
    take(mid.at[pl.ds(0, pairs - 1)], mid_recv)
    take(mid_edge, mide_recv)

    def fill_frame(f):
        for j in range(nh):
            place(act1, (f, slice(1, 1 + rows)), j, mid[j * ns:(j + 1) * ns, f],
                  mid_edge[j * ns:(j + 1) * ns, f], terms[j])

    pl.when(s > 0)(lambda: fill_frame(0))
    fill_frame(1)
    for dt in range(3):
        loads[3 + dt].wait()
    half = rows * width
    oldest = taps(lambda di, dj: act1[dj, 0, di:di + rows], w1, 0)
    both = taps(lambda di, dj: act1[dj, :, di:di + rows], w1, 1)
    newest = taps(lambda di, dj: act1[dj, 1, di:di + rows], w1, 2)
    shared = oldest + newest + first_conv_bias[...].reshape(1, chans)
    summed = jnp.concatenate([shared + both[:half], shared + both[half:]], axis=0)
    tile = summed.astype(BF16).reshape(2 * rows, width, chans)
    values = tile.astype(F32)
    hid_src[...] = tile
    hid_edge_src[...] = edge_of(values)
    own_stats(2, values)
    visit_all(functools.partial(send_stats, 2))
    for slot in (1, 0):
        def ring(slot=slot):
            steps = 1 - slot
            for d in range(0 if steps else 1, nh):
                there = {"seq": s + steps, "ch": wrap(h + d, nh), "col": k}
                send(hid_src, hid.at[slot, h], hid_send.at[slot], hid_recv.at[slot], there)
            for d in range(nh):
                there = {"seq": s + steps, "ch": wrap(h + d, nh), "col": other}
                send(hid_edge_src, hid_edge.at[slot, h], hide_send.at[slot], hide_recv.at[slot], there)
        near(1 - slot, ring)
    hid[1, h] = tile

    terms = norm_terms(2, 2 * rows * width * group_size * spread_over)
    for slot in (1, 0):
        def fill(slot=slot):
            if slot == 1:
                take(hid.at[slot, pl.ds(0, nh - 1)], hid_recv.at[slot])
            else:
                take(hid.at[slot], hid_recv.at[slot])
            take(hid_edge.at[slot], hide_recv.at[slot])
            for j in range(nh):
                for f in range(2):
                    part = slice(f * rows, (f + 1) * rows)
                    place(act2, (2 * slot + f, slice(1, 1 + rows)), j, hid[slot, j, part],
                          hid_edge[slot, j, part], terms[j])
        near(slot - 1, fill)
    mixed = None
    for dt in range(3):
        loads[6 + dt].wait()
        part = taps(lambda di, dj: act2[dj, dt:dt + 2, di:di + rows], w2, dt)
        mixed = part if mixed is None else mixed + part
    mixed = mixed + second_conv_bias[...].reshape(1, chans)
    kept = mid[pl.ds(h * ns, ns), 1].astype(F32).reshape(half, chans)
    for f in range(2):
        whole = kept + mixed[f * half:(f + 1) * half]
        out[f] = whole.astype(BF16).reshape(rows, width, chans)

    for step in range(3):
        take(stat.at[step, pl.ds(0, n - 1)], stat_send.at[step])
    take(params.at[pl.ds(0, nh - 1)], par_send)
    take(mid.at[pl.ds(0, pairs - 1)], mid_send)
    take(mid_edge, mide_send)
    for slot in range(3):
        def left(slot=slot):
            if slot == 1:
                take(lat.at[slot, pl.ds(0, nh - 1)], lat_send.at[slot])
            else:
                take(lat.at[slot], lat_send.at[slot])
            take(lat_edge.at[slot], late_send.at[slot])
        near(1 - slot, left)
    for slot in (1, 0):
        def left(slot=slot):
            if slot == 1:
                take(hid.at[slot, pl.ds(0, nh - 1)], hid_send.at[slot])
            else:
                take(hid.at[slot], hid_send.at[slot])
            take(hid_edge.at[slot], hide_send.at[slot])
        near(1 - slot, left)


def solution(mesh):
    ns, nh, nk = mesh.shape["seq"], mesh.shape["ch"], mesh.shape["col"]

    def body(
        latent,
        mid_gain, mid_bias, mid_weight, mid_conv_bias,
        first_gain, first_bias, first_weight, first_conv_bias,
        second_gain, second_bias, second_weight, second_conv_bias,
    ):
        frames, own_rows, width, chans = latent.shape
        assert nk == 2 and own_rows == 1 and frames == ns
        rows = ns
        full = chans * nh
        sizes = (ns, nh, nk, frames, width, chans, full // GROUPS)
        n, pairs = ns * nh * nk, ns * nh
        vmem = pl.BlockSpec(memory_space=pltpu.VMEM)
        hbm = pl.BlockSpec(memory_space=pl.ANY)
        dma = pltpu.SemaphoreType.DMA
        taps = mid_weight.shape
        return pl.pallas_call(
            functools.partial(kernel, sizes),
            out_shape=pltpu.VMEM((2, rows, width, chans), BF16),
            in_specs=[hbm] * 13,
            out_specs=vmem,
            scratch_shapes=[
                pltpu.VMEM(latent.shape, BF16), *[pltpu.VMEM((chans,), F32)] * 9, dma((10,)),
                pltpu.VMEM(taps, BF16), pltpu.VMEM(taps, BF16), pltpu.VMEM(taps, BF16), dma((3, 3)),
                pltpu.VMEM((3, frames + 2, 3, width, full), F32),
                pltpu.VMEM((3, 2, rows + 2, width, full), F32),
                pltpu.VMEM((3, 4, rows + 2, width, full), F32),
                pltpu.VMEM((nh, 8, chans), F32),
                pltpu.VMEM((3, n, 2, chans), F32),
                pltpu.VMEM((max(8, 2 * nh), chans), F32),
                pltpu.VMEM((chans, chans), BF16),
                pltpu.VMEM((3, nh, frames, width, chans), BF16),
                pltpu.VMEM((frames, 1, chans), F32),
                pltpu.VMEM((3, nh, frames, 1, chans), F32),
                pltpu.VMEM((frames + 1, width, chans), BF16),
                pltpu.VMEM((frames + 1, 1, chans), F32),
                pltpu.VMEM((pairs, 2, width, chans), BF16),
                pltpu.VMEM((pairs, 2, 1, chans), F32),
                pltpu.VMEM((2 * rows, width, chans), BF16),
                pltpu.VMEM((2 * rows, 1, chans), F32),
                pltpu.VMEM((2, nh, 2 * rows, width, chans), BF16),
                pltpu.VMEM((2, nh, 2 * rows, 1, chans), F32),
                dma, dma, dma((3,)), dma((3,)),
                dma((3,)), dma((3,)), dma((3,)), dma((3,)),
                dma, dma, dma, dma,
                dma((2,)), dma((2,)), dma((2,)), dma((2,)),
            ],
            compiler_params=pltpu.CompilerParams(
                collective_id=0, has_side_effects=True, vmem_limit_bytes=60 * 1024 * 1024
            ),
        )(
            latent,
            mid_gain, mid_bias, mid_conv_bias,
            first_gain, first_bias, first_conv_bias,
            second_gain, second_bias, second_conv_bias,
            mid_weight, first_weight, second_weight,
        )

    vector, weight = P("ch"), P(None, None, None, None, "ch")
    in_specs = (P("grp", "seq", "col", "ch"),) + (vector, vector, weight, vector) * 3
    out_specs = P(("grp", "seq"), None, "col", "ch")
    return jax.shard_map(body, mesh=mesh, in_specs=in_specs, out_specs=out_specs, check_vma=False)
```

```python
import functools

import jax
import jax.numpy as jnp
from jax import lax
from jax.experimental import pallas as pl
from jax.experimental.pallas import tpu as pltpu
from jax.sharding import PartitionSpec as P

GROUPS = 32
MESH = pl.DeviceIdType.MESH
F32 = jnp.float32
BF16 = jnp.bfloat16


def each(count, visit):
    if count <= 4:
        for i in range(count):
            visit(i)
    else:
        lax.fori_loop(0, count, lambda i, carry: (visit(i), carry)[1], 0)


def kernel(
    sizes,
    *refs,
):
    smalls, (mid_weight, first_weight, second_weight), (out,) = refs[:10], refs[10:13], refs[13:14]
    latent, *vectors = refs[14:24]
    (mid_gain, mid_bias, mid_conv_bias, first_gain, first_bias, first_conv_bias,
     second_gain, second_bias, second_conv_bias) = vectors
    (
    small_sem,
    w0, w1, w2, w_sem,
    act0, act1, act2,
    params, stat, packed, group_ref,
    lat, lat_edge_src, lat_edge,
    mid_src, mid_edge_src, mid, mid_edge,
    hid_src, hid_edge_src, hid, hid_edge,
    par_send, par_recv, stat_send, stat_recv,
    lat_send, lat_recv, late_send, late_recv,
    mid_send, mid_recv, mide_send, mide_recv,
    hid_send, hid_recv, hide_send, hide_recv,
    ) = refs[24:]
    ns, nh, nk, frames, width, chans, group_size = sizes
    rows = ns
    n, pairs, spread_over = ns * nh * nk, ns * nh, ns * nk
    s, h, k = lax.axis_index("seq"), lax.axis_index("ch"), lax.axis_index("col")
    other = 1 - k
    me = h * spread_over + s * nk + k

    def wrap(index, count):
        return jnp.where(index >= count, index - count, index)

    def visit_all(visit):
        down = s < ns // 2
        def one(i):
            row = jnp.where(down, ns - 1 - i, i)
            for dh in reversed(range(nh)):
                for dk in range(nk):
                    visit(row, dh, dk)
        each(ns, one)

    def others(row, dh, dk, act):
        if dh == 0 and dk == 0:
            pl.when(row != s)(act)
        else:
            act()

    def place_of(row, dh, dk):
        return {"seq": row, "ch": wrap(h + dh, nh), "col": k if dk == 0 else other}

    barrier = pltpu.get_barrier_semaphore()

    def greet(row, dh, dk):
        others(row, dh, dk, lambda: pl.semaphore_signal(
            barrier, inc=1, device_id=place_of(row, dh, dk), device_id_type=MESH))

    visit_all(greet)
    small_loads = []
    for i, (source, target) in enumerate(zip(smalls, [latent] + vectors)):
        load = pltpu.make_async_copy(source, target, small_sem.at[i])
        load.start()
        small_loads.append(load)

    def send(src, dst, send_sem, recv_sem, where):
        pltpu.make_async_remote_copy(
            src_ref=src, dst_ref=dst, send_sem=send_sem, recv_sem=recv_sem,
            device_id=where, device_id_type=MESH,
        ).start()

    def take(ref, sem):
        pltpu.make_async_copy(ref, ref, sem).wait()

    def own_stats(step, values):
        flat = values.reshape(-1, chans)
        stat[step, me, 0:1, :] = jnp.sum(flat, axis=0, keepdims=True)
        stat[step, me, 1:2, :] = jnp.sum(flat * flat, axis=0, keepdims=True)

    def send_stats(step, row, dh, dk):
        others(row, dh, dk, lambda: send(
            stat.at[step, me], stat.at[step, me], stat_send.at[step], stat_recv.at[step],
            place_of(row, dh, dk)))

    def edge_of(values):
        return jnp.where(k == 0, values[:, width - 1:width, :], values[:, 0:1, :])

    for load in small_loads:
        load.wait()

    tile = latent[...].reshape(frames, width, chans)
    values = tile.astype(F32)
    lat[1, h] = tile
    lat_edge_src[...] = edge_of(values)
    own_stats(0, values)
    for row, ref in enumerate((mid_gain, mid_bias, first_gain, first_bias, second_gain, second_bias)):
        params[h, row:row + 1, :] = ref[...].reshape(1, chans)

    pl.semaphore_wait(barrier, n - 1)

    visit_all(functools.partial(send_stats, 0))
    for d in range(1, nh):
        there = {"seq": s, "ch": wrap(h + d, nh), "col": k}
        send(params.at[h], params.at[h], par_send, par_recv, there)

    def near(steps, ring):
        if steps == 0:
            ring()
        else:
            pl.when((s + steps >= 0) & (s + steps < ns))(ring)

    for slot in range(3):
        def ring(slot=slot):
            steps = 1 - slot
            for d in range(0 if steps else 1, nh):
                there = {"seq": s + steps, "ch": wrap(h + d, nh), "col": k}
                send(lat.at[1, h], lat.at[slot, h], lat_send.at[slot], lat_recv.at[slot], there)
            for d in range(nh):
                there = {"seq": s + steps, "ch": wrap(h + d, nh), "col": other}
                send(lat_edge_src, lat_edge.at[slot, h], late_send.at[slot], late_recv.at[slot], there)
        near(1 - slot, ring)

    loads = []
    for c, (source, target) in enumerate(((mid_weight, w0), (first_weight, w1), (second_weight, w2))):
        for dt in range(3):
            load = pltpu.make_async_copy(source.at[dt], target.at[dt], w_sem.at[c, dt])
            load.start()
            loads.append(load)

    act0[...] = jnp.zeros_like(act0)
    act1[...] = jnp.zeros_like(act1)
    act2[...] = jnp.zeros_like(act2)
    packed[...] = jnp.zeros_like(packed)
    mid_src[0] = jnp.zeros((width, chans), BF16)
    mid_edge_src[0] = jnp.zeros((1, chans), F32)
    here = lax.broadcasted_iota(jnp.int32, (chans, chans), 0) // group_size
    there = lax.broadcasted_iota(jnp.int32, (chans, chans), 1) // group_size
    group_ref[...] = jnp.where(here == there, 1.0, 0.0).astype(BF16)

    def norm_terms(step, samples):
        take(stat.at[step, pl.ds(0, n - 1)], stat_recv.at[step])
        for j in range(nh):
            packed[2 * j:2 * j + 2, :] = jnp.sum(stat[step, j * spread_over:(j + 1) * spread_over], axis=0)
        exact = packed[...]
        high = exact.astype(BF16)
        rest = exact - high.astype(F32)
        middle = rest.astype(BF16)
        low = (rest - middle.astype(F32)).astype(BF16)
        group = group_ref[...]
        total = sum(jnp.dot(part, group, preferred_element_type=F32) for part in (low, middle, high))
        terms = []
        for j in range(nh):
            mean = total[2 * j:2 * j + 1] / samples
            square = total[2 * j + 1:2 * j + 2] / samples
            inverse = 1.0 / jnp.sqrt(square - mean * mean + 0.01)
            gain = params[j, 2 * step:2 * step + 1, :]
            shift = params[j, 2 * step + 1:2 * step + 2, :]
            terms.append((mean, inverse * gain, shift))
        return terms

    def activate(values, term):
        mean, scale, shift = term
        scaled = (values.astype(F32) - mean) * scale + shift
        return scaled / (1.0 + jnp.exp(-scaled))

    def place(target, index, j, values, edge, term):
        centre = activate(values, term)
        side = activate(edge, term)
        left = jnp.where(k == 1, side, 0.0)
        right = jnp.where(k == 0, side, 0.0)
        column = lax.broadcasted_iota(jnp.int32, centre.shape, 1)
        lanes = slice(j * chans, (j + 1) * chans)
        before = jnp.where(column == 0, left, pltpu.roll(centre, 1, 1))
        after = jnp.where(column == width - 1, right, pltpu.roll(centre, width - 1, 1))
        for dj, moved in enumerate((before, centre, after)):
            target[(dj,) + index + (slice(None), lanes)] = moved

    def taps(window, weight, dt):
        total = None
        for di in range(3):
            for dj in range(3):
                lhs = window(di, dj)
                lhs = lhs.reshape(-1, lhs.shape[-1]).astype(BF16)
                part = jnp.dot(lhs, weight[dt, di, dj], preferred_element_type=F32)
                total = part if total is None else total + part
        return total

    take(params.at[pl.ds(0, nh - 1)], par_recv)
    terms = norm_terms(0, frames * width * group_size * spread_over)
    for slot in range(3):
        def fill(slot=slot):
            if slot == 1:
                take(lat.at[slot, pl.ds(0, nh - 1)], lat_recv.at[slot])
            else:
                take(lat.at[slot], lat_recv.at[slot])
            take(lat_edge.at[slot], late_recv.at[slot])
            for j in range(nh):
                place(act0, (slice(2, 2 + frames), slot), j, lat[slot, j], lat_edge[slot, j], terms[j])
        near(slot - 1, fill)
    mixed = None
    for dt in range(3):
        loads[dt].wait()
        part = taps(lambda di, dj: act0[dj, dt:dt + frames, di], w0, dt)
        mixed = part if mixed is None else mixed + part
    summed = values.reshape(-1, chans) + mixed + mid_conv_bias[...].reshape(1, chans)
    tile = summed.astype(BF16).reshape(frames, width, chans)
    values = tile.astype(F32)
    mid_src[1:1 + frames] = tile
    mid_edge_src[1:1 + frames] = edge_of(values)
    own_stats(1, values)
    slot_here = h * ns + s

    def send_mid(row, dh, dk):
        send_stats(1, row, dh, dk)
        if dk == 0:
            others(row, dh, dk, lambda: send(
                mid_src.at[pl.ds(row, 2)], mid.at[slot_here], mid_send, mid_recv, place_of(row, dh, dk)))
        else:
            send(mid_edge_src.at[pl.ds(row, 2)], mid_edge.at[slot_here], mide_send, mide_recv,
                 place_of(row, dh, dk))

    visit_all(send_mid)
    mid[slot_here] = mid_src[pl.ds(s, 2)]

    terms = norm_terms(1, frames * width * group_size * spread_over)
    take(mid.at[pl.ds(0, pairs - 1)], mid_recv)
    take(mid_edge, mide_recv)

    def fill_frame(f):
        for j in range(nh):
            place(act1, (f, slice(1, 1 + rows)), j, mid[j * ns:(j + 1) * ns, f],
                  mid_edge[j * ns:(j + 1) * ns, f], terms[j])

    pl.when(s > 0)(lambda: fill_frame(0))
    fill_frame(1)
    for dt in range(3):
        loads[3 + dt].wait()
    half = rows * width
    oldest = taps(lambda di, dj: act1[dj, 0, di:di + rows], w1, 0)
    both = taps(lambda di, dj: act1[dj, :, di:di + rows], w1, 1)
    newest = taps(lambda di, dj: act1[dj, 1, di:di + rows], w1, 2)
    shared = oldest + newest + first_conv_bias[...].reshape(1, chans)
    summed = jnp.concatenate([shared + both[:half], shared + both[half:]], axis=0)
    tile = summed.astype(BF16).reshape(2 * rows, width, chans)
    values = tile.astype(F32)
    hid_src[...] = tile
    hid_edge_src[...] = edge_of(values)
    own_stats(2, values)
    visit_all(functools.partial(send_stats, 2))
    for slot in (1, 0):
        def ring(slot=slot):
            steps = 1 - slot
            for d in range(0 if steps else 1, nh):
                there = {"seq": s + steps, "ch": wrap(h + d, nh), "col": k}
                send(hid_src, hid.at[slot, h], hid_send.at[slot], hid_recv.at[slot], there)
            for d in range(nh):
                there = {"seq": s + steps, "ch": wrap(h + d, nh), "col": other}
                send(hid_edge_src, hid_edge.at[slot, h], hide_send.at[slot], hide_recv.at[slot], there)
        near(1 - slot, ring)
    hid[1, h] = tile

    terms = norm_terms(2, 2 * rows * width * group_size * spread_over)
    for slot in (1, 0):
        def fill(slot=slot):
            if slot == 1:
                take(hid.at[slot, pl.ds(0, nh - 1)], hid_recv.at[slot])
            else:
                take(hid.at[slot], hid_recv.at[slot])
            take(hid_edge.at[slot], hide_recv.at[slot])
            for j in range(nh):
                for f in range(2):
                    part = slice(f * rows, (f + 1) * rows)
                    place(act2, (2 * slot + f, slice(1, 1 + rows)), j, hid[slot, j, part],
                          hid_edge[slot, j, part], terms[j])
        near(slot - 1, fill)
    mixed = None
    for dt in range(3):
        loads[6 + dt].wait()
        part = taps(lambda di, dj: act2[dj, dt:dt + 2, di:di + rows], w2, dt)
        mixed = part if mixed is None else mixed + part
    mixed = mixed + second_conv_bias[...].reshape(1, chans)
    kept = mid[pl.ds(h * ns, ns), 1].astype(F32).reshape(half, chans)
    for f in range(2):
        whole = kept + mixed[f * half:(f + 1) * half]
        out[f] = whole.astype(BF16).reshape(rows, width, chans)

    for step in range(3):
        take(stat.at[step, pl.ds(0, n - 1)], stat_send.at[step])
    take(params.at[pl.ds(0, nh - 1)], par_send)
    take(mid.at[pl.ds(0, pairs - 1)], mid_send)
    take(mid_edge, mide_send)
    for slot in range(3):
        def left(slot=slot):
            if slot == 1:
                take(lat.at[slot, pl.ds(0, nh - 1)], lat_send.at[slot])
            else:
                take(lat.at[slot], lat_send.at[slot])
            take(lat_edge.at[slot], late_send.at[slot])
        near(1 - slot, left)
    for slot in (1, 0):
        def left(slot=slot):
            if slot == 1:
                take(hid.at[slot, pl.ds(0, nh - 1)], hid_send.at[slot])
            else:
                take(hid.at[slot], hid_send.at[slot])
            take(hid_edge.at[slot], hide_send.at[slot])
        near(1 - slot, left)


def solution(mesh):
    ns, nh, nk = mesh.shape["seq"], mesh.shape["ch"], mesh.shape["col"]

    def body(
        latent,
        mid_gain, mid_bias, mid_weight, mid_conv_bias,
        first_gain, first_bias, first_weight, first_conv_bias,
        second_gain, second_bias, second_weight, second_conv_bias,
    ):
        frames, own_rows, width, chans = latent.shape
        assert nk == 2 and own_rows == 1 and frames == ns
        rows = ns
        full = chans * nh
        sizes = (ns, nh, nk, frames, width, chans, full // GROUPS)
        n, pairs = ns * nh * nk, ns * nh
        vmem = pl.BlockSpec(memory_space=pltpu.VMEM)
        hbm = pl.BlockSpec(memory_space=pl.ANY)
        dma = pltpu.SemaphoreType.DMA
        taps = mid_weight.shape
        return pl.pallas_call(
            functools.partial(kernel, sizes),
            out_shape=pltpu.VMEM((2, rows, width, chans), BF16),
            in_specs=[hbm] * 13,
            out_specs=vmem,
            scratch_shapes=[
                pltpu.VMEM(latent.shape, BF16), *[pltpu.VMEM((chans,), F32)] * 9, dma((10,)),
                pltpu.VMEM(taps, BF16), pltpu.VMEM(taps, BF16), pltpu.VMEM(taps, BF16), dma((3, 3)),
                pltpu.VMEM((3, frames + 2, 3, width, full), F32),
                pltpu.VMEM((3, 2, rows + 2, width, full), F32),
                pltpu.VMEM((3, 4, rows + 2, width, full), F32),
                pltpu.VMEM((nh, 8, chans), F32),
                pltpu.VMEM((3, n, 2, chans), F32),
                pltpu.VMEM((max(8, 2 * nh), chans), F32),
                pltpu.VMEM((chans, chans), BF16),
                pltpu.VMEM((3, nh, frames, width, chans), BF16),
                pltpu.VMEM((frames, 1, chans), F32),
                pltpu.VMEM((3, nh, frames, 1, chans), F32),
                pltpu.VMEM((frames + 1, width, chans), BF16),
                pltpu.VMEM((frames + 1, 1, chans), F32),
                pltpu.VMEM((pairs, 2, width, chans), BF16),
                pltpu.VMEM((pairs, 2, 1, chans), F32),
                pltpu.VMEM((2 * rows, width, chans), BF16),
                pltpu.VMEM((2 * rows, 1, chans), F32),
                pltpu.VMEM((2, nh, 2 * rows, width, chans), BF16),
                pltpu.VMEM((2, nh, 2 * rows, 1, chans), F32),
                dma, dma, dma((3,)), dma((3,)),
                dma((3,)), dma((3,)), dma((3,)), dma((3,)),
                dma, dma, dma, dma,
                dma((2,)), dma((2,)), dma((2,)), dma((2,)),
            ],
            compiler_params=pltpu.CompilerParams(
                collective_id=0, has_side_effects=True, vmem_limit_bytes=60 * 1024 * 1024
            ),
        )(
            latent,
            mid_gain, mid_bias, mid_conv_bias,
            first_gain, first_bias, first_conv_bias,
            second_gain, second_bias, second_conv_bias,
            mid_weight, first_weight, second_weight,
        )

    vector, weight = P("ch"), P(None, None, None, None, "ch")
    in_specs = (P("grp", "seq", "col", "ch"),) + (vector, vector, weight, vector) * 3
    out_specs = P(("grp", "seq"), None, "col", "ch")
    return jax.shard_map(body, mesh=mesh, in_specs=in_specs, out_specs=out_specs, check_vma=False)
```
